32 devices in a mesh: dp: 4 (over x, y), tp: 8 (over z, core).
Axes of the slice: x: 2, y: 2, z: 4, core: 2. Of those that a mesh axis runs over, the one named last changes fastest.
Arguments:
- x: bfloat16 [3072, 12288], P(('dp', 'tp')), parts along dimension 0
- w_gate: bfloat16 [12288, 33792], P(None, 'tp')
- w_up: bfloat16 [12288, 33792], P(None, 'tp')
- w_down: bfloat16 [33792, 12288], P('tp')
Outputs:
- output: bfloat16 [3072, 12288], P(('dp', 'tp')), parts along dimension 0
There are 4 independent parts. The reference program is written for one: setup_inputs(seed, part) draws one part's arguments, and reference() takes and returns one part's arrays. A program takes and returns all parts, laid end to end along the dimension named above; an argument that names none is the same for every part.
All inputs are finite; a program needn't handle non-finite values.
Results may differ from the reference program's by a relative error of at most 0.016.
Values are sent between devices in bfloat16 or wider.
A program may use at most 2 GiB of HBM per device.

```python
import jax
import jax.numpy as jnp

ROWS = 768
D = 12288
FF = 33792


def setup_inputs(seed: int = 0, part: int = 0) -> dict:
    kx, kg, ku, kd = jax.random.split(jax.random.key(seed), 4)
    drawn = {
        "x": jax.random.normal(jax.random.fold_in(kx, part), (ROWS, D), jnp.float32),
        "w_gate": jax.random.normal(kg, (D, FF), jnp.float32) * D**-0.5,
        "w_up": jax.random.normal(ku, (D, FF), jnp.float32) * D**-0.5,
        "w_down": jax.random.normal(kd, (FF, D), jnp.float32) * FF**-0.5,
    }
    return {k: v.astype(jnp.bfloat16) for k, v in drawn.items()}


def reference(x, w_gate, w_up, w_down):
    gate = jnp.dot(x, w_gate, preferred_element_type=jnp.float32)
    up = jnp.dot(x, w_up, preferred_element_type=jnp.float32)
    hidden = (jax.nn.silu(gate) * up).astype(jnp.bfloat16)
    return jnp.dot(hidden, w_down, preferred_element_type=jnp.float32).astype(jnp.bfloat16)
```

```python
import functools
import types

import jax
import jax.numpy as jnp
from jax import lax
from jax.experimental import pallas as pl
from jax.experimental.pallas import tpu as pltpu
from jax.sharding import PartitionSpec as P

BF, F32 = jnp.bfloat16, jnp.float32
LA, LR = 2, 3
RING = 4
SR = 3
A0 = 2


def config(rows_per_device, depth, hidden, rows, kc):
    c = types.SimpleNamespace()
    c.X, c.D, c.H = rows_per_device, depth, hidden
    c.KC, c.NK = kc, depth // kc
    c.NT = hidden // 128
    assert c.NT * 128 == hidden and c.NK * kc == depth
    c.UN = depth // 256
    c.NU = depth // 512
    c.rows = rows
    c.S = len(rows)
    c.off = [[sum(r[:i]) for i in range(5)] for r in rows]
    c.M = c.off[0][4]
    assert all(o[4] == c.M for o in c.off)
    c.RM = max(max(r) for r in rows)
    for z in range(4):
        assert sum(r[z] for r in rows) == c.X
    held = [[z for z in range(4) if r[z]] for r in rows]
    c.zmin, c.zmax = [h[0] for h in held], [h[-1] for h in held]
    c.ag_lag = [LA * max(max(z - c.zmin[s], c.zmax[s] - z) for z in range(4)) for s in range(c.S)]
    c.rs_lag = [A0 + LR * max(max(z, 3 - z) for z in held[s]) for s in range(c.S)]
    c.TA = [c.NK + lag + RING for lag in c.ag_lag]
    c.TR = [c.NU + lag + SR for lag in c.rs_lag]
    m = c.M
    c.scratch = [
        pltpu.VMEM((c.NK, 2 * m, kc), BF),
        pltpu.VMEM((c.NT, 2 * m, 256), F32),
        pltpu.VMEM((c.UN, m, 256), F32),
        pltpu.VMEM((2 * m, hidden), BF),
        pltpu.VMEM((2, kc, hidden), BF),
        pltpu.VMEM((2, kc, hidden), BF),
        pltpu.VMEM((4, hidden, 256), BF),
        pltpu.VMEM((SR, m, 512), BF),
        pltpu.VMEM((4, m, 512), BF),
        pltpu.VMEM((3, c.RM, 512), BF),
        pltpu.VMEM((2, SR, m, 512), BF),
        pltpu.VMEM((2, c.RM, 512), BF),
        pltpu.SemaphoreType.DMA((2, 2)),
        pltpu.SemaphoreType.DMA((4,)),
        pltpu.SemaphoreType.DMA,
        *[pltpu.SemaphoreType.DMA((3, c.NK)) for _ in rows],
        pltpu.SemaphoreType.DMA((3, RING)),
        *[pltpu.SemaphoreType.DMA((3, c.NU)) for _ in rows],
        pltpu.SemaphoreType.DMA((3, SR)),
        pltpu.SemaphoreType.DMA((7,)),
        pltpu.SemaphoreType.DMA((2,)),
        pltpu.SemaphoreType.REGULAR,
    ]
    return c


def kernel(c, x, wg, wu, wd, y, *refs):
    S, m = c.S, c.M
    land = [refs[3 * s : 3 * s + 3] for s in range(S)]
    refs = refs[3 * S :]
    (xs, acc, kept, hid, gw, uw, dw, ss, lin, fin, out, yst, gsem, dsem, xsem), refs = refs[:15], refs[15:]
    agr, ags, rsr = refs[:S], refs[S], refs[S + 1 : 2 * S + 1]
    rss, lsem, ysem, free = refs[2 * S + 1 :]

    tp = lax.axis_index("tp")
    z, core = tp // 2, lax.rem(tp, 2)
    sib = {"tp": z * 2 + 1 - core}

    def dev(zz):
        return {"tp": zz * 2 + core}

    def within(i, n):
        return jnp.logical_and(i >= 0, i < n)

    def repeat(lo, hi, f):
        lax.fori_loop(lo, hi, lambda t, _: (f(t), 0)[1], 0)

    def at_chip(f):
        for zz in range(4):
            pl.when(z == zz)(functools.partial(f, zz))

    def remote(src, dst, send, recv, to):
        return pltpu.make_async_remote_copy(
            src_ref=src, dst_ref=dst, send_sem=send, recv_sem=recv,
            device_id=to, device_id_type=pl.DeviceIdType.MESH,
        )

    def gcopies(k, slot):
        at = pl.ds(pl.multiple_of(k * c.KC, c.KC), c.KC)
        return [
            pltpu.make_async_copy(wg.at[at, :], gw.at[slot], gsem.at[0, slot]),
            pltpu.make_async_copy(wu.at[at, :], uw.at[slot], gsem.at[1, slot]),
        ]

    def dcopy(n, slot):
        at = pl.ds(pl.multiple_of(n * 256, 256), 256)
        return pltpu.make_async_copy(wd.at[:, at], dw.at[slot], dsem.at[slot])

    def ag_rows(s, zz, way):
        o = c.off[s]
        return [(0, o[min(zz + 1, 4)]), (o[zz], m), (0, m)][way]

    def ag_copy(s, zz, way, j):
        a, b = ag_rows(s, zz, way)
        to = [lambda: dev(zz + 1), lambda: dev(zz - 1), lambda: sib][way]()
        dst = pl.ds(m, m) if way == 2 else pl.ds(a, b - a)
        return remote(
            xs.at[j, pl.ds(a, b - a), :], xs.at[j, dst, :],
            ags.at[way, lax.rem(j + 2 * RING, RING)], agr[s].at[way, j], to,
        )

    def ag_tick(s, tau):
        def at(zz):
            up, down = zz - c.zmin[s], c.zmax[s] - zz
            lags = [max(up, 0), max(down, 0), max(up, down)]
            for way in range(3):
                j = tau - LA * lags[way]
                a, b = ag_rows(s, zz, way)
                sends = b > a and (way == 2 or (zz < 3 if way == 0 else zz > 0))
                before = zz - 1 if way == 0 else zz + 1
                takes = way < 2 and 0 <= before < 4
                if takes:
                    a, b = ag_rows(s, before, way)
                    takes = b > a

                def take(j=j, way=way, before=before):
                    ag_copy(s, before, way, j).wait_recv()

                def sent(j=j, way=way):
                    ag_copy(s, zz, way, j - RING).wait_send()

                def send(j=j, way=way):
                    ag_copy(s, zz, way, j).start()

                if takes:
                    pl.when(within(j, c.NK))(take)
                if sends:
                    pl.when(within(j - RING, c.NK))(sent)
                    pl.when(within(j, c.NK))(send)

        at_chip(at)

    def rs_rows(s, zz, way):
        o = c.off[s]
        return [(o[min(zz + 1, 4)], m), (0, o[zz]), (0, m)][way]

    def rs_copy(s, zz, way, u):
        a, b = rs_rows(s, zz, way)
        rows = pl.ds(a, b - a)
        slot = lax.rem(u + 2 * SR, SR)
        to = [lambda: dev(zz + 1), lambda: dev(zz - 1), lambda: sib][way]()
        src = ss.at[slot, rows, :] if way == 2 else out.at[way, slot, rows, :]
        return remote(src, land[s][way].at[u, rows, :], rss.at[way, slot], rsr[s].at[way, u], to)

    def rs_takes(s, zz, way):
        before = zz - 1 if way == 0 else zz + 1
        if not 0 <= before < 4:
            return False
        a, b = rs_rows(s, before, way)
        return b > a

    def rs_sends(s, zz, way):
        a, b = rs_rows(s, zz, way)
        return b > a and (zz < 3 if way == 0 else zz > 0)

    def rs_unit(s, zz, part, tau):
        return tau - A0 - LR * [zz, 3 - zz, max(zz, 3 - zz)][part]

    def rs_loads(s, zz, part, u):
        sb = land[s][2]
        if part == 2:
            rows, n = pl.ds(c.off[s][zz], c.rows[s][zz]), pl.ds(0, c.rows[s][zz])
            cps = [(sb.at[u, rows, :], fin.at[2, n, :], 6)]
            for way in range(2):
                if rs_takes(s, zz, way):
                    cps.append((land[s][way].at[u, rows, :], fin.at[way, n, :], 4 + way))
        else:
            a, b = rs_rows(s, zz, part)
            rows = pl.ds(a, b - a)
            cps = [(sb.at[u, rows, :], lin.at[2 + part, rows, :], 2 + part)]
            if rs_takes(s, zz, part):
                cps.append((land[s][part].at[u, rows, :], lin.at[part, rows, :], part))
        return [pltpu.make_async_copy(p, q, lsem.at[i]) for p, q, i in cps]

    def rs_parts(s, zz):
        return [p for p in range(3) if (c.rows[s][zz] > 0 if p == 2 else rs_sends(s, zz, p))]

    def rs_first(s, tau):
        @pl.when(within(tau - A0, c.NU))
        def _():
            rs_copy(s, 0, 2, tau - A0).wait_recv()

        def at(zz):
            for way in range(2):
                if rs_takes(s, zz, way):
                    u = rs_unit(s, zz, way, tau)

                    @pl.when(within(u, c.NU))
                    def _(u=u, way=way):
                        rs_copy(s, zz - 1 if way == 0 else zz + 1, way, u).wait_recv()

            for part in rs_parts(s, zz):
                u = rs_unit(s, zz, part, tau)

                @pl.when(within(u, c.NU))
                def _(u=u, part=part):
                    for cp in rs_loads(s, zz, part, u):
                        cp.start()

        at_chip(at)

    def rs_second(s, tau):
        def at(zz):
            for part in rs_parts(s, zz):
                u = rs_unit(s, zz, part, tau)
                if part == 2:
                    a, b = c.off[s][zz], c.off[s][zz + 1]
                    ins, to = (fin.at[2], fin.at[0], fin.at[1]), yst.at[lax.rem(u + 4, 2)]
                    takes, lo, n = [rs_takes(s, zz, 0), rs_takes(s, zz, 1)], a, 2
                else:
                    a, b = rs_rows(s, zz, part)
                    ins, to = (lin.at[2 + part], lin.at[part]), out.at[part, lax.rem(u + 2 * SR, SR)]
                    takes, lo, n = [rs_takes(s, zz, part)], 0, SR

                @pl.when(within(u - n, c.NU))
                def _(u=u, part=part):
                    if part == 2:
                        ystore(s, zz, u - 2).wait()
                    else:
                        rs_copy(s, zz, part, u - SR).wait_send()

                @pl.when(within(u, c.NU))
                def _(u=u, part=part, a=a, b=b, ins=ins, to=to, takes=takes, lo=lo):
                    for cp in rs_loads(s, zz, part, u):
                        cp.wait()
                    rows = pl.ds(a - lo, b - a)
                    for h in range(2):
                        cols = pl.ds(256 * h, 256)
                        v = kept[2 * u + h, pl.ds(a, b - a), :] + ins[0][rows, cols].astype(F32)
                        for i, take in enumerate(takes):
                            if take:
                                v = v + ins[1 + i][rows, cols].astype(F32)
                        to[rows, cols] = v.astype(BF)

            for part in rs_parts(s, zz):
                u = rs_unit(s, zz, part, tau)

                @pl.when(within(u, c.NU))
                def _(u=u, part=part):
                    if part == 2:
                        ystore(s, zz, u).start()
                    else:
                        rs_copy(s, zz, part, u).start()

        at_chip(at)

    def ystore(s, zz, u):
        r, r0 = c.rows[s][zz], sum(c.rows[t][zz] for t in range(s))
        slot = lax.rem(u + 4, 2)
        at = (pl.ds(r0, r), pl.ds(pl.multiple_of(u * 512, 512), 512))
        return pltpu.make_async_copy(yst.at[slot, pl.ds(0, r), :], y.at[at], ysem.at[slot])

    def gate_up(s, before, after):
        def chunk(k):
            slot = lax.rem(k, 2)
            for cp in gcopies(k, slot):
                cp.wait()
            ag_copy(s, 0, 2, k).wait_recv()
            if s + 1 < S:
                for cp in gcopies(lax.rem(k + 1, c.NK), 1 - slot):
                    cp.start()
            else:

                @pl.when(k + 1 < c.NK)
                def _():
                    for cp in gcopies(k + 1, 1 - slot):
                        cp.start()

            before(k)
            for t in range(c.NT):
                cols = pl.ds(t * 128, 128)
                w = jnp.concatenate([gw[slot, :, cols], uw[slot, :, cols]], axis=1)
                acc[t] += jnp.dot(xs[k], w, preferred_element_type=F32)
            after(k)

        repeat(0, c.NK, chunk)

    def activate():
        def act(t):
            g, u = acc[t, :, pl.ds(0, 128)], acc[t, :, pl.ds(128, 128)]
            h = (g * jax.nn.sigmoid(g)) * u
            hid[:, pl.ds(pl.multiple_of(t * 128, 128), 128)] = h.astype(BF)
            acc[t] = jnp.zeros((2 * m, 256), F32)

        repeat(0, c.NT, act)

    def down(s, before, after):
        def unit(u):
            half = 2 * lax.rem(u, 2)
            for h in range(2):
                dcopy(0, half + h).wait()
            for h in range(2):
                if s + 1 < S:
                    dcopy(lax.rem(2 * u + 2 + h, c.UN), 2 - half + h).start()
                else:

                    @pl.when(u + 1 < c.NU)
                    def _(h=h):
                        dcopy(2 * u + 2 + h, 2 - half + h).start()

            @pl.when(u >= SR)
            def _():
                rs_copy(s, 0, 2, u - SR).wait_send()

            before(u)
            slot = lax.rem(u, SR)
            for h in range(2):
                v = jnp.dot(hid[...], dw[half + h], preferred_element_type=F32)
                kept[2 * u + h] = v[:m]
                ss[slot, :, pl.ds(256 * h, 256)] = v[m:].astype(BF)
            rs_copy(s, 0, 2, u).start()
            after(u)

        repeat(0, c.NU, unit)
        for i in range(SR):
            rs_copy(s, 0, 2, c.NU - SR + i).wait_send()

    def own(s, zz, j):
        r0 = sum(c.rows[t][zz] for t in range(s))
        at = (pl.ds(r0, c.rows[s][zz]), pl.ds(pl.multiple_of(j * c.KC, c.KC), c.KC))
        return pltpu.make_async_copy(x.at[at], xs.at[j, pl.ds(c.off[s][zz], c.rows[s][zz]), :], xsem)

    def own_start(s):
        def at(zz):
            if c.rows[s][zz]:
                repeat(0, c.NK, lambda j: own(s, zz, j).start())

        at_chip(at)

    def own_wait(s):
        def at(zz):
            if c.rows[s][zz]:
                part = xs.at[:, pl.ds(c.off[s][zz], c.rows[s][zz]), :]
                pltpu.make_async_copy(part, part, xsem).wait()

        at_chip(at)

    def tell(sem):
        def signal(to):
            pl.semaphore_signal(sem, inc=1, device_id=to, device_id_type=pl.DeviceIdType.MESH)

        signal(sib)
        pl.when(z < 3)(lambda: signal(dev(z + 1)))
        pl.when(z > 0)(lambda: signal(dev(z - 1)))

    def hear(sem):
        pl.semaphore_wait(sem, 1 + (z < 3).astype(jnp.int32) + (z > 0).astype(jnp.int32))

    tell(pltpu.get_barrier_semaphore())
    own_start(0)
    for cp in gcopies(0, 0):
        cp.start()
    for n in range(2):
        dcopy(n, n).start()

    def clear(t):
        acc[t] = jnp.zeros((2 * m, 256), F32)

    own_wait(0)
    hear(pltpu.get_barrier_semaphore())
    na, nd = c.ag_lag[0] + 2, c.NU // 2
    repeat(0, 2, lambda t: ag_tick(0, t))
    repeat(0, c.NT, clear)
    repeat(2, na, lambda t: ag_tick(0, t))
    nothing = lambda t: None
    gate_up(0, nothing, lambda k: ag_tick(0, k + na))
    repeat(c.NK + na, c.TA[0], lambda t: ag_tick(0, t))
    tell(free)
    own_start(1)
    activate()

    def before(u):
        @pl.when(u == 0)
        def _():
            own_wait(1)
            hear(free)

        pl.when(lax.rem(u, 2) == 0)(lambda: ag_tick(1, u // 2))
        pl.when(lax.rem(u, 2) == 1)(lambda: rs_first(0, u // 2))

    down(0, before, lambda u: pl.when(lax.rem(u, 2) == 1)(lambda: rs_second(0, u // 2)))

    def after(k):
        rs_second(0, k + nd)
        ag_tick(1, k + nd)

    gate_up(1, lambda k: rs_first(0, k + nd), after)

    def both(s):
        def run(t):
            rs_first(s, t)
            rs_second(s, t)
        return run

    repeat(c.NK + nd, max(c.TA[1], c.NK + nd), lambda t: ag_tick(1, t))
    repeat(c.NK + nd, max(c.TR[0], c.NK + nd), both(0))
    activate()
    down(1, lambda u: rs_first(1, u), lambda u: rs_second(1, u))
    repeat(c.NU, c.TR[1], both(1))


def block(c, x, wg, wu, wd):
    lands = [jax.ShapeDtypeStruct((c.NU, c.M, 512), BF) for _ in range(3 * c.S)]
    hbm = pl.BlockSpec(memory_space=pltpu.HBM)
    outs = pl.pallas_call(
        functools.partial(kernel, c),
        out_shape=[jax.ShapeDtypeStruct((c.X, c.D), BF), *lands],
        in_specs=[hbm] * 4,
        out_specs=[hbm] * (1 + len(lands)),
        scratch_shapes=c.scratch,
        compiler_params=pltpu.CompilerParams(
            collective_id=0, has_side_effects=True, vmem_limit_bytes=67043328
        ),
        name="mlp",
    )(x, wg, wu, wd)
    return outs[0]


ROWS = [[32,64,64,32],[64,32,32,64]]


def solution(mesh):
    def step(x, w_gate, w_up, w_down):
        c = config(x.shape[0], x.shape[1], w_gate.shape[1], ROWS, 512)
        return block(c, x, w_gate, w_up, w_down)

    return jax.shard_map(
        step,
        mesh=mesh,
        in_specs=(P(("dp", "tp"), None), P(None, "tp"), P(None, "tp"), P("tp", None)),
        out_specs=P(("dp", "tp"), None),
        check_vma=False,
    )
```

```python
import functools
import types

import jax
import jax.numpy as jnp
from jax import lax
from jax.experimental import pallas as pl
from jax.experimental.pallas import tpu as pltpu
from jax.sharding import PartitionSpec as P

BF, F32 = jnp.bfloat16, jnp.float32
LA = 2
LR = (2, 2)
RING = 4
SR = 3
A0 = (0, 1)


def config(rows_per_device, depth, hidden, rows, kc):
    c = types.SimpleNamespace()
    c.X, c.D, c.H = rows_per_device, depth, hidden
    c.KC, c.NK = kc, depth // kc
    c.NT = hidden // 128
    assert c.NT * 128 == hidden and c.NK * kc == depth
    c.UN = depth // 256
    c.NU = depth // 512
    c.rows = rows
    c.S = len(rows)
    c.off = [[sum(r[:i]) for i in range(5)] for r in rows]
    c.M = c.off[0][4]
    assert all(o[4] == c.M for o in c.off)
    c.RM = max(max(r) for r in rows)
    for z in range(4):
        assert sum(r[z] for r in rows) == c.X
    held = [[z for z in range(4) if r[z]] for r in rows]
    c.zmin, c.zmax = [h[0] for h in held], [h[-1] for h in held]
    c.ag_lag = [LA * max(max(z - c.zmin[s], c.zmax[s] - z) for z in range(4)) for s in range(c.S)]
    c.rs_lag = [A0[s] + LR[s] * max(max(z, 3 - z) for z in held[s]) for s in range(c.S)]
    c.TA = [c.NK + lag + RING for lag in c.ag_lag]
    c.TR = [c.NU + lag + SR for lag in c.rs_lag]
    m = c.M
    c.scratch = [
        pltpu.VMEM((c.NK, 2 * m, kc), BF),
        pltpu.VMEM((c.NT, 2 * m, 256), F32),
        pltpu.VMEM((c.UN, m, 256), F32),
        pltpu.VMEM((2 * m, hidden), BF),
        pltpu.VMEM((2, kc, hidden), BF),
        pltpu.VMEM((2, kc, hidden), BF),
        pltpu.VMEM((5, hidden, 256), BF),
        pltpu.VMEM((SR, m, 512), BF),
        pltpu.VMEM((4, m, 512), BF),
        pltpu.VMEM((3, c.RM, 512), BF),
        pltpu.VMEM((2, SR, m, 512), BF),
        pltpu.VMEM((2, c.RM, 512), BF),
        pltpu.SemaphoreType.DMA((2, 2)),
        pltpu.SemaphoreType.DMA((5,)),
        pltpu.SemaphoreType.DMA,
        *[pltpu.SemaphoreType.DMA((3, c.NK)) for _ in rows],
        pltpu.SemaphoreType.DMA((3, RING)),
        *[pltpu.SemaphoreType.DMA((3, c.NU)) for _ in rows],
        pltpu.SemaphoreType.DMA((3, SR)),
        pltpu.SemaphoreType.DMA((7,)),
        pltpu.SemaphoreType.DMA((2,)),
        pltpu.SemaphoreType.REGULAR((2,)),
    ]
    return c


def kernel(c, x, wg, wu, wd, y, *refs):
    S, m = c.S, c.M
    land, refs = refs[:3], refs[3:]
    (xs, acc, kept, hid, gw, uw, dw, ss, lin, fin, out, yst, gsem, dsem, xsem), refs = refs[:15], refs[15:]
    agr, ags, rsr = refs[:S], refs[S], refs[S + 1 : 2 * S + 1]
    rss, lsem, ysem, free = refs[2 * S + 1 :]

    tp = lax.axis_index("tp")
    z, core = tp // 2, lax.rem(tp, 2)
    sib = {"tp": z * 2 + 1 - core}

    def dev(zz):
        return {"tp": zz * 2 + core}

    def within(i, n):
        return jnp.logical_and(i >= 0, i < n)

    def repeat(lo, hi, f):
        lax.fori_loop(lo, hi, lambda t, _: (f(t), 0)[1], 0)

    def at_chip(f):
        for zz in range(4):
            pl.when(z == zz)(functools.partial(f, zz))

    def remote(src, dst, send, recv, to):
        return pltpu.make_async_remote_copy(
            src_ref=src, dst_ref=dst, send_sem=send, recv_sem=recv,
            device_id=to, device_id_type=pl.DeviceIdType.MESH,
        )

    def gcopies(k, slot):
        at = pl.ds(pl.multiple_of(k * c.KC, c.KC), c.KC)
        return [
            pltpu.make_async_copy(wg.at[at, :], gw.at[slot], gsem.at[0, slot]),
            pltpu.make_async_copy(wu.at[at, :], uw.at[slot], gsem.at[1, slot]),
        ]

    def dcopy(n, slot):
        at = pl.ds(pl.multiple_of(n * 256, 256), 256)
        return pltpu.make_async_copy(wd.at[:, at], dw.at[slot], dsem.at[slot])

    def ag_rows(s, zz, way):
        o = c.off[s]
        return [(0, o[min(zz + 1, 4)]), (o[zz], m), (0, m)][way]

    def ag_copy(s, zz, way, j):
        a, b = ag_rows(s, zz, way)
        to = [lambda: dev(zz + 1), lambda: dev(zz - 1), lambda: sib][way]()
        dst = pl.ds(m, m) if way == 2 else pl.ds(a, b - a)
        return remote(
            xs.at[j, pl.ds(a, b - a), :], xs.at[j, dst, :],
            ags.at[way, lax.rem(j + 2 * RING, RING)], agr[s].at[way, j], to,
        )

    def ag_tick(s, tau):
        def at(zz):
            up, down = zz - c.zmin[s], c.zmax[s] - zz
            lags = [max(up, 0), max(down, 0), max(up, down)]
            for way in range(3):
                j = tau - LA * lags[way]
                a, b = ag_rows(s, zz, way)
                sends = b > a and (way == 2 or (zz < 3 if way == 0 else zz > 0))
                before = zz - 1 if way == 0 else zz + 1
                takes = way < 2 and 0 <= before < 4
                if takes:
                    a, b = ag_rows(s, before, way)
                    takes = b > a

                def take(j=j, way=way, before=before):
                    ag_copy(s, before, way, j).wait_recv()

                def sent(j=j, way=way):
                    ag_copy(s, zz, way, j - RING).wait_send()

                def send(j=j, way=way):
                    ag_copy(s, zz, way, j).start()

                if takes:
                    pl.when(within(j, c.NK))(take)
                if sends:
                    pl.when(within(j - RING, c.NK))(sent)
                    pl.when(within(j, c.NK))(send)

        at_chip(at)

    def rs_rows(s, zz, way):
        o = c.off[s]
        return [(o[min(zz + 1, 4)], m), (0, o[zz]), (0, m)][way]

    def rs_copy(s, zz, way, u):
        a, b = rs_rows(s, zz, way)
        rows = pl.ds(a, b - a)
        slot = lax.rem(u + 2 * SR, SR)
        to = [lambda: dev(zz + 1), lambda: dev(zz - 1), lambda: sib][way]()
        src = ss.at[slot, rows, :] if way == 2 else out.at[way, slot, rows, :]
        return remote(src, landing(s, way, u, a, b), rss.at[way, slot], rsr[s].at[way, u], to)

    def landing(s, way, u, a, b, h=None):
        if s + 1 < S:
            return land[way].at[u, pl.ds(a, b - a), :]
        if way < 2:
            cols = pl.ds(0, 512) if h is None else pl.ds(256 * h, 256)
            return xs.at[u, pl.ds(way * m + a, b - a), cols]
        row, col = lax.rem(u // 8, 2) * (c.KC // 2), lax.rem(u, 8) * 512
        if h is not None:
            col = col + 256 * h
        cols = pl.ds(pl.multiple_of(col, 256), 512 if h is None else 256)
        return gw.at[u // 16, pl.ds(pl.multiple_of(row + a, 16), b - a), cols]

    def rs_takes(s, zz, way):
        before = zz - 1 if way == 0 else zz + 1
        if not 0 <= before < 4:
            return False
        a, b = rs_rows(s, before, way)
        return b > a

    def rs_sends(s, zz, way):
        a, b = rs_rows(s, zz, way)
        return b > a and (zz < 3 if way == 0 else zz > 0)

    def rs_unit(s, zz, part, tau):
        return tau - A0[s] - LR[s] * [zz, 3 - zz, max(zz, 3 - zz)][part]

    def rs_loads(s, zz, part, u):
        if s + 1 == S:
            return []
        sb = land[2]
        if part == 2:
            rows, n = pl.ds(c.off[s][zz], c.rows[s][zz]), pl.ds(0, c.rows[s][zz])
            cps = [(sb.at[u, rows, :], fin.at[2, n, :], 6)]
            for way in range(2):
                if rs_takes(s, zz, way):
                    cps.append((land[way].at[u, rows, :], fin.at[way, n, :], 4 + way))
        else:
            a, b = rs_rows(s, zz, part)
            rows = pl.ds(a, b - a)
            cps = [(sb.at[u, rows, :], lin.at[2 + part, rows, :], 2 + part)]
            if rs_takes(s, zz, part):
                cps.append((land[part].at[u, rows, :], lin.at[part, rows, :], part))
        return [pltpu.make_async_copy(p, q, lsem.at[i]) for p, q, i in cps]

    def rs_parts(s, zz):
        return [p for p in range(3) if (c.rows[s][zz] > 0 if p == 2 else rs_sends(s, zz, p))]

    def rs_first(s, tau):
        @pl.when(within(tau - A0[s], c.NU))
        def _():
            rs_copy(s, 0, 2, tau - A0[s]).wait_recv()

        def at(zz):
            for way in range(2):
                if rs_takes(s, zz, way):
                    u = rs_unit(s, zz, way, tau)

                    @pl.when(within(u, c.NU))
                    def _(u=u, way=way):
                        rs_copy(s, zz - 1 if way == 0 else zz + 1, way, u).wait_recv()

            for part in rs_parts(s, zz):
                u = rs_unit(s, zz, part, tau)

                @pl.when(within(u, c.NU))
                def _(u=u, part=part):
                    for cp in rs_loads(s, zz, part, u):
                        cp.start()

        at_chip(at)

    def rs_second(s, tau):
        def at(zz):
            for part in rs_parts(s, zz):
                u = rs_unit(s, zz, part, tau)
                if part == 2:
                    a, b = c.off[s][zz], c.off[s][zz + 1]
                    to, lo, n = yst.at[lax.rem(u + 4, 2)], a, 2
                    takes = [2] + [w for w in range(2) if rs_takes(s, zz, w)]
                else:
                    a, b = rs_rows(s, zz, part)
                    to, lo, n = out.at[part, lax.rem(u + 2 * SR, SR)], 0, SR
                    takes = [2] + [part] * rs_takes(s, zz, part)

                @pl.when(within(u - n, c.NU))
                def _(u=u, part=part):
                    if part == 2:
                        ystore(s, zz, u - 2).wait()
                    else:
                        rs_copy(s, zz, part, u - SR).wait_send()

                @pl.when(within(u, c.NU))
                def _(u=u, part=part, a=a, b=b, to=to, takes=takes, lo=lo):
                    for cp in rs_loads(s, zz, part, u):
                        cp.wait()
                    for h in range(2):
                        cols = pl.ds(256 * h, 256)
                        v = kept[2 * u + h, pl.ds(a, b - a), :]
                        for way in takes:
                            if s + 1 == S:
                                w = landing(s, way, u, a, b, h)[...]
                            elif part == 2:
                                w = fin[way, pl.ds(0, b - a), cols]
                            else:
                                w = lin[part + (2 if way == 2 else 0), pl.ds(a, b - a), cols]
                            v = v + w.astype(F32)
                        to[pl.ds(a - lo, b - a), cols] = v.astype(BF)

            for part in rs_parts(s, zz):
                u = rs_unit(s, zz, part, tau)

                @pl.when(within(u, c.NU))
                def _(u=u, part=part):
                    if part == 2:
                        ystore(s, zz, u).start()
                    else:
                        rs_copy(s, zz, part, u).start()

        at_chip(at)

    def ystore(s, zz, u):
        r, r0 = c.rows[s][zz], sum(c.rows[t][zz] for t in range(s))
        slot = lax.rem(u + 4, 2)
        at = (pl.ds(r0, r), pl.ds(pl.multiple_of(u * 512, 512), 512))
        return pltpu.make_async_copy(yst.at[slot, pl.ds(0, r), :], y.at[at], ysem.at[slot])

    def gate_up(s, before, after):
        def chunk(k):
            slot = lax.rem(k, 2)
            for cp in gcopies(k, slot):
                cp.wait()
            ag_copy(s, 0, 2, k).wait_recv()
            if s + 1 < S:
                for cp in gcopies(lax.rem(k + 1, c.NK), 1 - slot):
                    cp.start()
            else:

                @pl.when(k + 1 < c.NK)
                def _():
                    for cp in gcopies(k + 1, 1 - slot):
                        cp.start()

            before(k)
            for t in range(c.NT):
                cols = pl.ds(t * 128, 128)
                w = jnp.concatenate([gw[slot, :, cols], uw[slot, :, cols]], axis=1)
                acc[t] += jnp.dot(xs[k], w, preferred_element_type=F32)
            after(k)

        repeat(0, c.NK, chunk)

    def activate(s):
        def act(t):
            g, u = acc[t, :, pl.ds(0, 128)], acc[t, :, pl.ds(128, 128)]
            h = (g * jax.nn.sigmoid(g)) * u
            hid[:, pl.ds(pl.multiple_of(t * 128, 128), 128)] = h.astype(BF)
            if s + 1 < S:
                acc[t] = jnp.zeros((2 * m, 256), F32)

        repeat(0, c.NT, act)

    def down(s, before, after):
        def unit(u):
            n = s * c.UN + 2 * u
            for h in range(2):
                dcopy(0, lax.rem(n + h, 5)).wait()
            for h in range(3, 5):
                if s + 1 < S:
                    dcopy(lax.rem(2 * u + h, c.UN), lax.rem(n + h, 5)).start()
                else:

                    @pl.when(2 * u + h < c.UN)
                    def _(h=h):
                        dcopy(2 * u + h, lax.rem(n + h, 5)).start()

            @pl.when(u >= SR)
            def _():
                rs_copy(s, 0, 2, u - SR).wait_send()

            before(u)
            slot = lax.rem(u, SR)
            for h in range(2):
                v = jnp.dot(hid[...], dw[lax.rem(n + h, 5)], preferred_element_type=F32)
                kept[2 * u + h] = v[:m]
                ss[slot, :, pl.ds(256 * h, 256)] = v[m:].astype(BF)
            rs_copy(s, 0, 2, u).start()
            after(u)

        repeat(0, c.NU, unit)
        for i in range(SR):
            rs_copy(s, 0, 2, c.NU - SR + i).wait_send()

    def own(s, zz, j):
        r0 = sum(c.rows[t][zz] for t in range(s))
        at = (pl.ds(r0, c.rows[s][zz]), pl.ds(pl.multiple_of(j * c.KC, c.KC), c.KC))
        return pltpu.make_async_copy(x.at[at], xs.at[j, pl.ds(c.off[s][zz], c.rows[s][zz]), :], xsem)

    def own_start(s):
        def at(zz):
            if c.rows[s][zz]:
                repeat(0, c.NK, lambda j: own(s, zz, j).start())

        at_chip(at)

    def own_wait(s):
        def at(zz):
            if c.rows[s][zz]:
                part = xs.at[:, pl.ds(c.off[s][zz], c.rows[s][zz]), :]
                pltpu.make_async_copy(part, part, xsem).wait()

        at_chip(at)

    def tell(sem):
        def signal(to):
            pl.semaphore_signal(sem, inc=1, device_id=to, device_id_type=pl.DeviceIdType.MESH)

        signal(sib)
        pl.when(z < 3)(lambda: signal(dev(z + 1)))
        pl.when(z > 0)(lambda: signal(dev(z - 1)))

    def hear(sem):
        pl.semaphore_wait(sem, 1 + (z < 3).astype(jnp.int32) + (z > 0).astype(jnp.int32))

    tell(pltpu.get_barrier_semaphore())
    own_start(0)
    for cp in gcopies(0, 0):
        cp.start()
    for n in range(3):
        dcopy(n, n).start()

    def clear(t):
        acc[t] = jnp.zeros((2 * m, 256), F32)

    own_wait(0)
    hear(pltpu.get_barrier_semaphore())
    na, nd = c.ag_lag[0] + 2, c.NU // 2
    repeat(0, 2, lambda t: ag_tick(0, t))
    repeat(0, c.NT, clear)
    repeat(2, na - 1, lambda t: ag_tick(0, t))
    nothing = lambda t: None

    def after0(k):
        pl.when(k == 0)(lambda: ag_tick(0, na - 1))
        ag_tick(0, k + na)

    gate_up(0, nothing, after0)
    repeat(c.NK + na, c.TA[0], lambda t: ag_tick(0, t))
    tell(free.at[0])
    own_start(1)
    activate(0)

    def before(u):
        @pl.when(u == 0)
        def _():
            own_wait(1)
            hear(free.at[0])

        gathers = jnp.logical_and(lax.rem(u, 2) == 0, lax.rem(u, 8) != 6)
        pl.when(gathers)(lambda: ag_tick(1, u // 8 * 3 + lax.rem(u, 8) // 2))
        pl.when(lax.rem(u, 2) == 1)(lambda: rs_first(0, u // 2))

    down(0, before, lambda u: pl.when(lax.rem(u, 2) == 1)(lambda: rs_second(0, u // 2)))

    ng = 3 * c.NU // 8
    assert ng > c.ag_lag[1] + 1
    paced = 3 * c.NK // 4
    rs_on = lambda k: jnp.logical_or(k >= paced, lax.rem(k, 3) != 2)
    rs_at = lambda k: nd + jnp.where(k < paced, k - (k + 1) // 3, k - (paced + 1) // 3)

    def after(k):
        pl.when(rs_on(k))(lambda: rs_second(0, rs_at(k)))
        ag_tick(1, ng + k)

    gate_up(1, lambda k: pl.when(rs_on(k))(lambda: rs_first(0, rs_at(k))), after)

    def both(s):
        def run(t):
            rs_first(s, t)
            rs_second(s, t)
        return run

    ag_done, rs_done = ng + c.NK, nd + c.NK - (paced + 1) // 3
    assert ag_done >= c.NK + c.ag_lag[1]
    repeat(ag_done, c.TA[1], lambda t: ag_tick(1, t))
    repeat(rs_done, max(c.TR[0], rs_done), both(0))
    tell(free.at[1])
    activate(1)

    down(1, lambda u: pl.when(u == 0)(lambda: hear(free.at[1])), both(1))
    repeat(c.NU, c.TR[1], both(1))


def block(c, x, wg, wu, wd):
    lands = [jax.ShapeDtypeStruct((c.NU, c.M, 512), BF) for _ in range(3)]
    hbm = pl.BlockSpec(memory_space=pltpu.HBM)
    outs = pl.pallas_call(
        functools.partial(kernel, c),
        out_shape=[jax.ShapeDtypeStruct((c.X, c.D), BF), *lands],
        in_specs=[hbm] * 4,
        out_specs=[hbm] * (1 + len(lands)),
        scratch_shapes=c.scratch,
        compiler_params=pltpu.CompilerParams(
            collective_id=0, has_side_effects=True, vmem_limit_bytes=67043328
        ),
        name="mlp",
    )(x, wg, wu, wd)
    return outs[0]


ROWS = [[32,64,64,32],[64,32,32,64]]


def solution(mesh):
    def step(x, w_gate, w_up, w_down):
        c = config(x.shape[0], x.shape[1], w_gate.shape[1], ROWS, 512)
        return block(c, x, w_gate, w_up, w_down)

    return jax.shard_map(
        step,
        mesh=mesh,
        in_specs=(P(("dp", "tp"), None), P(None, "tp"), P(None, "tp"), P("tp", None)),
        out_specs=P(("dp", "tp"), None),
        check_vma=False,
    )
```

```python
import functools
import types

import jax
import jax.numpy as jnp
from jax import lax
from jax.experimental import pallas as pl
from jax.experimental.pallas import tpu as pltpu
from jax.sharding import PartitionSpec as P

BF, F32 = jnp.bfloat16, jnp.float32
LA = 2
LR = (2, 2)
RING = 4
SR = 3
A0 = (0, 1)


def config(rows_per_device, depth, hidden, rows, kc):
    c = types.SimpleNamespace()
    c.X, c.D, c.H = rows_per_device, depth, hidden
    c.KC, c.NK = kc, depth // kc
    c.NT = hidden // 128
    assert c.NT * 128 == hidden and c.NK * kc == depth
    c.UN = depth // 256
    c.NU = depth // 512
    c.rows = rows
    c.S = len(rows)
    c.off = [[sum(r[:i]) for i in range(5)] for r in rows]
    c.M = c.off[0][4]
    assert all(o[4] == c.M for o in c.off)
    c.RM = max(max(r) for r in rows)
    for z in range(4):
        assert sum(r[z] for r in rows) == c.X
    held = [[z for z in range(4) if r[z]] for r in rows]
    c.zmin, c.zmax = [h[0] for h in held], [h[-1] for h in held]
    c.ag_lag = [LA * max(max(z - c.zmin[s], c.zmax[s] - z) for z in range(4)) for s in range(c.S)]
    c.rs_lag = [A0[s] + LR[s] * max(max(z, 3 - z) for z in held[s]) for s in range(c.S)]
    c.TA = [c.NK + lag + RING for lag in c.ag_lag]
    c.TR = [c.NU + lag + SR for lag in c.rs_lag]
    m = c.M
    c.scratch = [
        pltpu.VMEM((c.NK, 2 * m, kc), BF),
        pltpu.VMEM((c.NT, 2 * m, 256), F32),
        pltpu.VMEM((c.UN, m, 256), F32),
        pltpu.VMEM((2 * m, hidden), BF),
        pltpu.VMEM((2, kc, hidden), BF),
        pltpu.VMEM((2, kc, hidden), BF),
        pltpu.VMEM((5, hidden, 256), BF),
        pltpu.VMEM((SR, m, 512), BF),
        pltpu.VMEM((4, m, 512), BF),
        pltpu.VMEM((3, c.RM, 512), BF),
        pltpu.VMEM((2, SR, m, 512), BF),
        pltpu.VMEM((2, c.RM, 512), BF),
        pltpu.SemaphoreType.DMA((2, 2)),
        pltpu.SemaphoreType.DMA((5,)),
        pltpu.SemaphoreType.DMA,
        *[pltpu.SemaphoreType.DMA((3, max(c.NK, c.NU))) for _ in rows],
        pltpu.SemaphoreType.DMA((3, RING)),
        pltpu.SemaphoreType.DMA((3, SR)),
        pltpu.SemaphoreType.DMA((7,)),
        pltpu.SemaphoreType.DMA((2,)),
        pltpu.SemaphoreType.REGULAR((2,)),
    ]
    return c


def kernel(c, x, wg, wu, wd, y, *refs):
    S, m = c.S, c.M
    land, refs = refs[:3], refs[3:]
    (xs, acc, kept, hid, gw, uw, dw, ss, lin, fin, out, yst, gsem, dsem, xsem), refs = refs[:15], refs[15:]
    agr, ags = refs[:S], refs[S]
    rsr = agr
    rss, lsem, ysem, free = refs[S + 1 :]

    tp = lax.axis_index("tp")
    z, core = tp // 2, lax.rem(tp, 2)
    sib = {"tp": z * 2 + 1 - core}

    def dev(zz):
        return {"tp": zz * 2 + core}

    def within(i, n):
        return jnp.logical_and(i >= 0, i < n)

    def repeat(lo, hi, f):
        lax.fori_loop(lo, hi, lambda t, _: (f(t), 0)[1], 0)

    def at_chip(f):
        for zz in range(4):
            pl.when(z == zz)(functools.partial(f, zz))

    def remote(src, dst, send, recv, to):
        return pltpu.make_async_remote_copy(
            src_ref=src, dst_ref=dst, send_sem=send, recv_sem=recv,
            device_id=to, device_id_type=pl.DeviceIdType.MESH,
        )

    def gcopies(k, slot):
        at = pl.ds(pl.multiple_of(k * c.KC, c.KC), c.KC)
        return [
            pltpu.make_async_copy(wg.at[at, :], gw.at[slot], gsem.at[0, slot]),
            pltpu.make_async_copy(wu.at[at, :], uw.at[slot], gsem.at[1, slot]),
        ]

    def dcopy(n, slot):
        at = pl.ds(pl.multiple_of(n * 256, 256), 256)
        return pltpu.make_async_copy(wd.at[:, at], dw.at[slot], dsem.at[slot])

    def ag_rows(s, zz, way):
        o = c.off[s]
        return [(0, o[min(zz + 1, 4)]), (o[zz], m), (0, m)][way]

    def ag_copy(s, zz, way, j):
        a, b = ag_rows(s, zz, way)
        to = [lambda: dev(zz + 1), lambda: dev(zz - 1), lambda: sib][way]()
        dst = pl.ds(m, m) if way == 2 else pl.ds(a, b - a)
        return remote(
            xs.at[j, pl.ds(a, b - a), :], xs.at[j, dst, :],
            ags.at[way, lax.rem(j + 2 * RING, RING)], agr[s].at[way, j], to,
        )

    def ag_tick(s, tau):
        def at(zz):
            up, down = zz - c.zmin[s], c.zmax[s] - zz
            lags = [max(up, 0), max(down, 0), max(up, down)]
            for way in range(3):
                j = tau - LA * lags[way]
                a, b = ag_rows(s, zz, way)
                sends = b > a and (way == 2 or (zz < 3 if way == 0 else zz > 0))
                before = zz - 1 if way == 0 else zz + 1
                takes = way < 2 and 0 <= before < 4
                if takes:
                    a, b = ag_rows(s, before, way)
                    takes = b > a

                def take(j=j, way=way, before=before):
                    ag_copy(s, before, way, j).wait_recv()

                def sent(j=j, way=way):
                    ag_copy(s, zz, way, j - RING).wait_send()

                def send(j=j, way=way):
                    ag_copy(s, zz, way, j).start()

                if takes:
                    pl.when(within(j, c.NK))(take)
                if sends:
                    pl.when(within(j - RING, c.NK))(sent)
                    pl.when(within(j, c.NK))(send)

        at_chip(at)

    def rs_rows(s, zz, way):
        o = c.off[s]
        return [(o[min(zz + 1, 4)], m), (0, o[zz]), (0, m)][way]

    def rs_copy(s, zz, way, u):
        a, b = rs_rows(s, zz, way)
        rows = pl.ds(a, b - a)
        slot = lax.rem(u + 2 * SR, SR)
        to = [lambda: dev(zz + 1), lambda: dev(zz - 1), lambda: sib][way]()
        src = ss.at[slot, rows, :] if way == 2 else out.at[way, slot, rows, :]
        return remote(src, landing(s, way, u, a, b), rss.at[way, slot], rsr[s].at[way, u], to)

    def landing(s, way, u, a, b, h=None):
        if s + 1 < S:
            return land[way].at[u, pl.ds(a, b - a), :]
        if way < 2:
            cols = pl.ds(0, 512) if h is None else pl.ds(256 * h, 256)
            return xs.at[u, pl.ds(way * m + a, b - a), cols]
        row, col = lax.rem(u // 8, 2) * (c.KC // 2), lax.rem(u, 8) * 512
        if h is not None:
            col = col + 256 * h
        cols = pl.ds(pl.multiple_of(col, 256), 512 if h is None else 256)
        return gw.at[u // 16, pl.ds(pl.multiple_of(row + a, 16), b - a), cols]

    def rs_takes(s, zz, way):
        before = zz - 1 if way == 0 else zz + 1
        if not 0 <= before < 4:
            return False
        a, b = rs_rows(s, before, way)
        return b > a

    def rs_sends(s, zz, way):
        a, b = rs_rows(s, zz, way)
        return b > a and (zz < 3 if way == 0 else zz > 0)

    def rs_unit(s, zz, part, tau):
        return tau - A0[s] - LR[s] * [zz, 3 - zz, max(zz, 3 - zz)][part]

    def rs_loads(s, zz, part, u):
        if s + 1 == S:
            return []
        sb = land[2]
        if part == 2:
            rows, n = pl.ds(c.off[s][zz], c.rows[s][zz]), pl.ds(0, c.rows[s][zz])
            cps = [(sb.at[u, rows, :], fin.at[2, n, :], 6)]
            for way in range(2):
                if rs_takes(s, zz, way):
                    cps.append((land[way].at[u, rows, :], fin.at[way, n, :], 4 + way))
        else:
            a, b = rs_rows(s, zz, part)
            rows = pl.ds(a, b - a)
            cps = [(sb.at[u, rows, :], lin.at[2 + part, rows, :], 2 + part)]
            if rs_takes(s, zz, part):
                cps.append((land[part].at[u, rows, :], lin.at[part, rows, :], part))
        return [pltpu.make_async_copy(p, q, lsem.at[i]) for p, q, i in cps]

    def rs_parts(s, zz):
        return [p for p in range(3) if (c.rows[s][zz] > 0 if p == 2 else rs_sends(s, zz, p))]

    def rs_first(s, tau):
        @pl.when(within(tau - A0[s], c.NU))
        def _():
            rs_copy(s, 0, 2, tau - A0[s]).wait_recv()

        def at(zz):
            for way in range(2):
                if rs_takes(s, zz, way):
                    u = rs_unit(s, zz, way, tau)

                    @pl.when(within(u, c.NU))
                    def _(u=u, way=way):
                        rs_copy(s, zz - 1 if way == 0 else zz + 1, way, u).wait_recv()

            for part in rs_parts(s, zz):
                u = rs_unit(s, zz, part, tau)

                @pl.when(within(u, c.NU))
                def _(u=u, part=part):
                    for cp in rs_loads(s, zz, part, u):
                        cp.start()

        at_chip(at)

    def rs_second(s, tau):
        def at(zz):
            for part in rs_parts(s, zz):
                u = rs_unit(s, zz, part, tau)
                if part == 2:
                    a, b = c.off[s][zz], c.off[s][zz + 1]
                    to, lo, n = yst.at[lax.rem(u + 4, 2)], a, 2
                    takes = [2] + [w for w in range(2) if rs_takes(s, zz, w)]
                else:
                    a, b = rs_rows(s, zz, part)
                    to, lo, n = out.at[part, lax.rem(u + 2 * SR, SR)], 0, SR
                    takes = [2] + [part] * rs_takes(s, zz, part)

                @pl.when(within(u - n, c.NU))
                def _(u=u, part=part):
                    if part == 2:
                        ystore(s, zz, u - 2).wait()
                    else:
                        rs_copy(s, zz, part, u - SR).wait_send()

                @pl.when(within(u, c.NU))
                def _(u=u, part=part, a=a, b=b, to=to, takes=takes, lo=lo):
                    for cp in rs_loads(s, zz, part, u):
                        cp.wait()
                    for h in range(2):
                        cols = pl.ds(256 * h, 256)
                        v = kept[2 * u + h, pl.ds(a, b - a), :]
                        for way in takes:
                            if s + 1 == S:
                                w = landing(s, way, u, a, b, h)[...]
                            elif part == 2:
                                w = fin[way, pl.ds(0, b - a), cols]
                            else:
                                w = lin[part + (2 if way == 2 else 0), pl.ds(a, b - a), cols]
                            v = v + w.astype(F32)
                        to[pl.ds(a - lo, b - a), cols] = v.astype(BF)

            for part in rs_parts(s, zz):
                u = rs_unit(s, zz, part, tau)

                @pl.when(within(u, c.NU))
                def _(u=u, part=part):
                    if part == 2:
                        ystore(s, zz, u).start()
                    else:
                        rs_copy(s, zz, part, u).start()

        at_chip(at)

    def ystore(s, zz, u):
        r, r0 = c.rows[s][zz], sum(c.rows[t][zz] for t in range(s))
        slot = lax.rem(u + 4, 2)
        at = (pl.ds(r0, r), pl.ds(pl.multiple_of(u * 512, 512), 512))
        return pltpu.make_async_copy(yst.at[slot, pl.ds(0, r), :], y.at[at], ysem.at[slot])

    def gate_up(s, before, after):
        def chunk(k, last=False):
            slot = lax.rem(k, 2)
            for cp in gcopies(k, slot):
                cp.wait()
            ag_copy(s, 0, 2, k).wait_recv()
            if s + 1 < S:
                for cp in gcopies(lax.rem(k + 1, c.NK), 1 - slot):
                    cp.start(priority=1)
            else:

                @pl.when(k + 1 < c.NK)
                def _():
                    for cp in gcopies(k + 1, 1 - slot):
                        cp.start(priority=1)

            before(k)
            for t in range(c.NT):
                cols = pl.ds(t * 128, 128)
                w = jnp.concatenate([gw[slot, :, cols], uw[slot, :, cols]], axis=1)
                v = acc[t] + jnp.dot(xs[k], w, preferred_element_type=F32)
                if not last:
                    acc[t] = v
                    continue
                g, u = v[:, :128], v[:, 128:]
                hid[:, cols] = ((g * jax.nn.sigmoid(g)) * u).astype(BF)
                if s + 1 < S:
                    acc[t] = jnp.zeros((2 * m, 256), F32)
            after(k)

        repeat(0, c.NK - 1, chunk)
        chunk(jnp.int32(c.NK - 1), True)

    def down(s, before, after):
        def unit(u):
            n = s * c.UN + 2 * u
            for h in range(2):
                dcopy(0, lax.rem(n + h, 5)).wait()
            for h in range(3, 5):
                if s + 1 < S:
                    dcopy(lax.rem(2 * u + h, c.UN), lax.rem(n + h, 5)).start(priority=1)
                else:

                    @pl.when(2 * u + h < c.UN)
                    def _(h=h):
                        dcopy(2 * u + h, lax.rem(n + h, 5)).start(priority=1)

            @pl.when(u >= SR)
            def _():
                rs_copy(s, 0, 2, u - SR).wait_send()

            before(u)
            slot = lax.rem(u, SR)
            for h in range(2):
                v = jnp.dot(hid[...], dw[lax.rem(n + h, 5)], preferred_element_type=F32)
                kept[2 * u + h] = v[:m]
                ss[slot, :, pl.ds(256 * h, 256)] = v[m:].astype(BF)
            rs_copy(s, 0, 2, u).start()
            after(u)

        repeat(0, c.NU, unit)
        for i in range(SR):
            rs_copy(s, 0, 2, c.NU - SR + i).wait_send()

    def own(s, zz, j):
        r0 = sum(c.rows[t][zz] for t in range(s))
        at = (pl.ds(r0, c.rows[s][zz]), pl.ds(pl.multiple_of(j * c.KC, c.KC), c.KC))
        return pltpu.make_async_copy(x.at[at], xs.at[j, pl.ds(c.off[s][zz], c.rows[s][zz]), :], xsem)

    def own_start(s):
        def at(zz):
            if c.rows[s][zz]:
                repeat(0, c.NK, lambda j: own(s, zz, j).start())

        at_chip(at)

    def own_wait(s):
        def at(zz):
            if c.rows[s][zz]:
                part = xs.at[:, pl.ds(c.off[s][zz], c.rows[s][zz]), :]
                pltpu.make_async_copy(part, part, xsem).wait()

        at_chip(at)

    def tell(sem):
        def signal(to):
            pl.semaphore_signal(sem, inc=1, device_id=to, device_id_type=pl.DeviceIdType.MESH)

        signal(sib)
        pl.when(z < 3)(lambda: signal(dev(z + 1)))
        pl.when(z > 0)(lambda: signal(dev(z - 1)))

    def hear(sem):
        pl.semaphore_wait(sem, 1 + (z < 3).astype(jnp.int32) + (z > 0).astype(jnp.int32))

    tell(pltpu.get_barrier_semaphore())
    own_start(0)
    for cp in gcopies(0, 0):
        cp.start()
    for n in range(3):
        dcopy(n, n).start()

    def clear(t):
        acc[t] = jnp.zeros((2 * m, 256), F32)

    own_wait(0)
    hear(pltpu.get_barrier_semaphore())
    na, nd = c.ag_lag[0] + 2, c.NU // 2
    repeat(0, 2, lambda t: ag_tick(0, t))
    repeat(0, c.NT, clear)
    repeat(2, na - 1, lambda t: ag_tick(0, t))
    nothing = lambda t: None

    def after0(k):
        pl.when(k == 0)(lambda: ag_tick(0, na - 1))
        ag_tick(0, k + na)

    gate_up(0, nothing, after0)
    repeat(c.NK + na, c.TA[0], lambda t: ag_tick(0, t))
    tell(free.at[0])
    own_start(1)

    def before(u):
        @pl.when(u == 0)
        def _():
            own_wait(1)
            hear(free.at[0])

        gathers = jnp.logical_and(lax.rem(u, 2) == 0, lax.rem(u, 8) != 6)
        pl.when(gathers)(lambda: ag_tick(1, u // 8 * 3 + lax.rem(u, 8) // 2))
        pl.when(lax.rem(u, 2) == 1)(lambda: rs_first(0, u // 2))

    down(0, before, lambda u: pl.when(lax.rem(u, 2) == 1)(lambda: rs_second(0, u // 2)))

    ng = 3 * c.NU // 8
    assert ng > c.ag_lag[1] + 1
    paced = 3 * c.NK // 4
    rs_on = lambda k: jnp.logical_or(k >= paced, lax.rem(k, 3) != 2)
    rs_at = lambda k: nd + jnp.where(k < paced, k - (k + 1) // 3, k - (paced + 1) // 3)

    def after(k):
        ag_tick(1, ng + k)
        pl.when(rs_on(k))(lambda: rs_second(0, rs_at(k)))

    gate_up(1, lambda k: pl.when(rs_on(k))(lambda: rs_first(0, rs_at(k))), after)

    def both(s):
        def run(t):
            rs_first(s, t)
            rs_second(s, t)
        return run

    ag_done, rs_done = ng + c.NK, nd + c.NK - (paced + 1) // 3
    assert ag_done >= c.NK + c.ag_lag[1]
    repeat(ag_done, c.TA[1], lambda t: ag_tick(1, t))
    repeat(rs_done, max(c.TR[0], rs_done), both(0))
    tell(free.at[1])

    down(1, lambda u: pl.when(u == 0)(lambda: hear(free.at[1])), both(1))
    repeat(c.NU, c.TR[1], both(1))


def block(c, x, wg, wu, wd):
    lands = [jax.ShapeDtypeStruct((c.NU, c.M, 512), BF) for _ in range(3)]
    hbm = pl.BlockSpec(memory_space=pltpu.HBM)
    outs = pl.pallas_call(
        functools.partial(kernel, c),
        out_shape=[jax.ShapeDtypeStruct((c.X, c.D), BF), *lands],
        in_specs=[hbm] * 4,
        out_specs=[hbm] * (1 + len(lands)),
        scratch_shapes=c.scratch,
        compiler_params=pltpu.CompilerParams(
            collective_id=0, has_side_effects=True, vmem_limit_bytes=67043328
        ),
        name="mlp",
    )(x, wg, wu, wd)
    return outs[0]


ROWS = [[32,64,64,32],[64,32,32,64]]


def solution(mesh):
    def step(x, w_gate, w_up, w_down):
        c = config(x.shape[0], x.shape[1], w_gate.shape[1], ROWS, 512)
        return block(c, x, w_gate, w_up, w_down)

    return jax.shard_map(
        step,
        mesh=mesh,
        in_specs=(P(("dp", "tp"), None), P(None, "tp"), P(None, "tp"), P("tp", None)),
        out_specs=P(("dp", "tp"), None),
        check_vma=False,
    )
```
